256 devices in a mesh: dp: 2 (over core), glob: 4 (over y), byte: 32 (over z, x).
Axes of the slice: x: 4, y: 4, z: 8, core: 2. Of those that a mesh axis runs over, the one named last changes fastest.
Arguments:
- byte_states: bfloat16 [2, 4096, 4096], P('dp', 'byte', 'glob'), may hold values from -8 to 8
- patch_start: int32 [2, 32, 32], P('dp'), may hold values from 0 to 128, as said below
- queries: bfloat16 [2, 1024, 2048], P('dp', 'byte', 'glob'), may hold values from -6 to 6
- grad_out: bfloat16 [2, 1024, 2048], P('dp', 'byte', 'glob'), may hold values from -6 to 6
- w_kv: bfloat16 [2, 4096, 512], P(None, 'byte', 'glob'), may hold values from -0.09375 to 0.09375
Outputs:
- attended: bfloat16 [2, 1024, 2048], P('dp', 'byte', 'glob')
- grad_queries: bfloat16 [2, 1024, 2048], P('dp', 'byte', 'glob')
- grad_bytes: bfloat16 [2, 4096, 4096], P('dp', 'byte', 'glob')
- grad_kv: float32 [2, 4096, 512], P(None, 'byte', 'glob')
The draws below stay inside these ranges and needn't reach their ends.
Inputs may be any that keep to these rules, and one draw needn't show every extreme that they name: Per shard: patch_start[s, 0] is 0, used slots come first with strictly rising starts, unused slots hold 128; a shard uses between 8 and 32 slots, and some shard of every draw uses all 32.
All inputs are finite; a program needn't handle non-finite values.
Results may differ from the reference program's by a relative error of at most 0.02.
Values may be sent and summed in bfloat16 or wider, within the bound.
No kernel may reach another device: no remote copies, remote signals or barrier semaphores. Data moves between devices by JAX's collectives and lax.ppermute only.
A program may use at most 64 MiB of HBM per device.

```python
import math
import jax
import jax.numpy as jnp
from jax import lax

D = 4096
HS = 128
HQ = 16
HK = 4
BYTE_DEV = 128
PMAX = 32
SEQS = 2
BYTES = 4096
SLOTS = 1024
N_BYTE = 32


def draw_byte_states(key, part):
    base = jax.random.normal(jax.random.fold_in(key, 11), (SEQS, BYTES, D), jnp.float32)
    base = jnp.clip(base, -8.0, 8.0)
    return base.astype(jnp.bfloat16)


def draw_patch_start(key, part):
    row_total = SEQS * N_BYTE
    first_key = jax.random.fold_in(key, 21)
    second_key = jax.random.fold_in(key, 22)
    third_key = jax.random.fold_in(key, 23)
    fourth_key = jax.random.fold_in(key, 24)
    drawn = jax.random.randint(first_key, (row_total,), PMAX // 4, 3 * PMAX // 4 + 1)
    filled = jax.random.randint(second_key, (row_total,), 0, 8) == 0
    forced = jax.random.randint(third_key, (), 0, row_total)
    filled = filled | (jnp.arange(row_total) == forced)
    used = jnp.where(filled, PMAX, drawn)
    scores = jax.random.randint(fourth_key, (row_total, BYTE_DEV - 1), 0, 1 << 16) * BYTE_DEV + jnp.arange(BYTE_DEV - 1)[None, :]
    unused, chosen = lax.top_k(scores, PMAX - 1)
    chosen = chosen + 1
    place = jnp.arange(PMAX - 1)[None, :]
    chosen = jnp.where(place < used[:, None] - 1, chosen, BYTE_DEV)
    chosen = jnp.sort(chosen, axis=1)
    starts = jnp.concatenate([jnp.zeros((row_total, 1), jnp.int32), chosen.astype(jnp.int32)], axis=1)
    return starts.reshape(SEQS, N_BYTE, PMAX)


def level_of(rng, shape, split, smallest, largest):
    def one(axis_at, shards_of):
        heights = jax.random.uniform(jax.random.fold_in(jax.random.fold_in(rng, 6), axis_at), (shards_of,), jnp.float32, smallest / len(split), largest / len(split))
        return jnp.repeat(jnp.exp(heights), shape[axis_at] // shards_of).reshape((-1,) + (1,) * (len(shape) - axis_at - 1))

    gain = one(*split[0])
    for cut in split[1:]:
        gain = gain * one(*cut)
    return gain


def centred(rng, dims, width, reach, shards=(), held_as=jnp.bfloat16):
    values = jax.random.normal(rng, dims, jnp.float32) * width
    if len(shards) > 0:
        values = level_of(rng, dims, shards, -0.22, 0.18) * values
    return jnp.clip(values, min=-reach, max=reach).astype(held_as)


def setup_inputs(seed: int = 0) -> dict:
    keys = jax.random.split(jax.random.key(seed), 6)
    return {
        "byte_states": draw_byte_states(jax.random.fold_in(keys[5], 71), 0),
        "patch_start": draw_patch_start(jax.random.fold_in(keys[5], 71), 0),
        "queries": centred(keys[2], (SEQS, SLOTS, HQ * HS), 1.0, 6.0, ((0, 2), (1, 32), (2, 4))),
        "grad_out": centred(keys[3], (SEQS, SLOTS, HQ * HS), 1.0, 6.0, ((0, 2), (1, 32), (2, 4))),
        "w_kv": centred(keys[4], (2, D, HK * HS), D ** -0.5, 0.09375, ((1, 32), (2, 4))),
    }


def segment_of(offsets, length):
    position = jnp.arange(length, dtype=jnp.int32)
    opened = (offsets[:, None] <= position[None, :]).astype(jnp.int32)
    return lax.optimization_barrier(jnp.sum(opened, axis=0)) - 1

def rounded(values_in):
    return lax.optimization_barrier(values_in.astype(jnp.bfloat16)).astype(jnp.float32)

def contract_rows(left, right):
    return lax.dot_general(left, right, (((0,), (0,)), ((), ())), preferred_element_type=jnp.float32)

def reference(byte_states, patch_start, queries, grad_out, w_kv):
    factor = 1.0 / math.sqrt(HS)
    group_size = HQ // HK
    slot_total = N_BYTE * PMAX
    key_ids = jnp.arange(slot_total, dtype=jnp.int32)
    slot_range = jnp.arange(PMAX, dtype=jnp.int32)
    shard_range = jnp.arange(N_BYTE, dtype=jnp.int32)
    grad_pair = jnp.zeros((D, 2 * HK * HS), jnp.float32)
    attended = []
    query_grads_all = []
    byte_grads = []
    for sequence in range(SEQS):
        states = byte_states[sequence].reshape(N_BYTE, BYTE_DEV, D)
        offsets = patch_start[sequence]
        segments = jax.vmap(lambda offset_row: segment_of(offset_row, BYTE_DEV))(offsets)
        members = (slot_range[None, :, None] == segments[:, None, :]).astype(jnp.float32)
        counts = jnp.maximum(lax.optimization_barrier(jnp.sum(members, axis=2)), 1.0)
        summed = jnp.einsum('spb,sbc->spc', members, states.astype(jnp.float32))
        pooled = (summed / counts[:, :, None]).astype(jnp.bfloat16).reshape(slot_total, D)
        usable = (offsets < BYTE_DEV).reshape(slot_total)
        seq_queries = queries[sequence]
        key_rows = jnp.dot(pooled, w_kv[0], preferred_element_type=jnp.float32).astype(jnp.bfloat16)
        value_rows = jnp.dot(pooled, w_kv[1], preferred_element_type=jnp.float32).astype(jnp.bfloat16)
        key_heads = key_rows.astype(jnp.float32).reshape(slot_total, HK, HS)
        value_heads = value_rows.astype(jnp.float32).reshape(slot_total, HK, HS)
        cotangent = grad_out[sequence]

        def per_shard(carried, shard_index):
            key_sum, value_sum = carried
            first = shard_index * PMAX
            local_query = lax.dynamic_slice_in_dim(seq_queries, first, PMAX, 0).astype(jnp.float32).reshape(PMAX, HK, group_size, HS)
            local_grad = lax.dynamic_slice_in_dim(cotangent, first, PMAX, 0).astype(jnp.float32).reshape(PMAX, HK, group_size, HS)
            live = lax.dynamic_slice_in_dim(usable, first, PMAX, 0).astype(jnp.float32)[:, None, None, None]
            query_ids = first + slot_range
            visible = (key_ids[None, :] <= query_ids[:, None]) & usable[None, :]
            scores = jnp.einsum('qcgd,kcd->cgqk', local_query, key_heads) * factor
            masked = jnp.where(visible, scores, -1e+30)
            highest = lax.optimization_barrier(jnp.max(masked, axis=-1, keepdims=True))
            raised = jnp.where(visible, jnp.exp(masked - highest), 0.0)
            totals = jnp.maximum(lax.optimization_barrier(jnp.sum(raised, axis=-1, keepdims=True)), 1.0)
            attention = raised / totals
            shortened = rounded(attention)
            mixed = jnp.einsum('cgqk,kcd->qcgd', shortened, value_heads)
            outputs = (mixed * live).astype(jnp.bfloat16).reshape(PMAX, HQ * HS)
            masked_grad = local_grad * live
            row_dots = jnp.einsum('qcgd,qcgd->cgq', masked_grad, mixed)
            prob_grad = jnp.einsum('qcgd,kcd->cgqk', masked_grad, value_heads)
            score_grad = rounded(attention * (prob_grad - row_dots[..., None]) * factor)
            query_grad = jnp.einsum('cgqk,kcd->qcgd', score_grad, key_heads).astype(jnp.bfloat16).reshape(PMAX, HQ * HS)
            key_part = jnp.einsum('cgqk,qcgd->kcd', score_grad, local_query).reshape(slot_total, HK * HS)
            value_part = jnp.einsum('cgqk,qcgd->kcd', shortened, masked_grad).reshape(slot_total, HK * HS)
            return ((key_sum + rounded(key_part), value_sum + rounded(value_part)), (outputs, query_grad))
        zero_keys = jnp.zeros((slot_total, HK * HS), jnp.float32)
        (key_sum, value_sum), (outputs, query_grads) = lax.scan(per_shard, (zero_keys, zero_keys), shard_range)
        attended.append(outputs.reshape(slot_total, HQ * HS))
        query_grads_all.append(query_grads.reshape(slot_total, HQ * HS))
        key_grad = key_sum.astype(jnp.bfloat16)
        value_grad = value_sum.astype(jnp.bfloat16)
        patch_grad = (jnp.dot(key_grad, w_kv[0].T, preferred_element_type=jnp.float32) + jnp.dot(value_grad, w_kv[1].T, preferred_element_type=jnp.float32)).astype(jnp.bfloat16)
        pool_grad = patch_grad.astype(jnp.float32) / counts.reshape(slot_total)[:, None]
        picked = (shard_range[:, None] * PMAX + segments).reshape(BYTES).astype(jnp.int32)
        byte_grads.append(jnp.take(pool_grad, picked, axis=0).astype(jnp.bfloat16))
        key_value = jnp.concatenate([key_grad, value_grad], axis=1)

        def weight_terms(pair_sum, shard_index):
            first = shard_index * PMAX
            pooled_piece = lax.dynamic_slice_in_dim(pooled, first, PMAX, 0)
            pair_piece = lax.dynamic_slice_in_dim(key_value, first, PMAX, 0)
            return (pair_sum + rounded(contract_rows(pooled_piece, pair_piece)), None)
        pair_add, unused = lax.scan(weight_terms, jnp.zeros((D, 2 * HK * HS), jnp.float32), shard_range)
        grad_pair = grad_pair + pair_add
    grad_kv = grad_pair.reshape(D, 2, HK * HS).transpose(1, 0, 2)
    return (jnp.stack(attended), jnp.stack(query_grads_all), jnp.stack(byte_grads), grad_kv)
```

```python
import math

import jax
import jax.numpy as jnp
from jax import lax
from jax.sharding import Mesh
from jax.sharding import PartitionSpec as P

HS = 128
BYTE = ("byte_0", "byte_1")


def gather_axes(value, axes, dim):
    out = value
    for number in range(len(axes) - 1, -1, -1):
        out = lax.all_gather(out, axes[number], axis=dim, tiled=True)
    return out


def copy_for_each(value, axis):
    copies = jnp.broadcast_to(value, (lax.axis_size(axis), *value.shape))
    return lax.all_to_all(copies, axis, split_axis=0, concat_axis=0, tiled=True)


def joined_along(pieces, dim):
    shape = list(pieces.shape[1:])
    shape[dim] *= pieces.shape[0]
    return jnp.moveaxis(pieces, 0, dim).reshape(shape)


def gathered_copies(value, axis, dim):
    pieces = copy_for_each(value, axis)
    return joined_along(pieces, dim)


def sent_together(arrays, axis, dim, along):
    both = jnp.concatenate(arrays, axis=along)
    out, at, done = (lax.all_gather(both, axis, axis=dim, tiled=True), 0, [])
    for a in arrays:
        done.append(lax.slice_in_dim(out, at, at + a.shape[along], axis=along))
        at += a.shape[along]
    return tuple(done)


def split_up(value, dim, count):
    shape = value.shape
    pieces = value.reshape(*shape[:dim], count, shape[dim] // count, *shape[dim + 1 :])
    return jnp.moveaxis(pieces, dim, 0)


def summed_on_arrival(value, axis, dim):
    count = lax.axis_size(axis)
    pieces = lax.all_to_all(split_up(value, dim, count), axis, 0, 0, tiled=True)
    return jnp.sum(pieces.astype(jnp.float32), axis=0)


def sent_together_2(arrays, axis, dim, along):
    ends, at = ([], 0)
    for a in arrays[:-1]:
        at += a.shape[along]
        ends.append(at)
    both = jnp.concatenate(arrays, axis=along)
    return tuple(jnp.split(summed_on_arrival(both, axis, dim), ends, axis=along))


def segment_of(offsets, length):
    position = jnp.arange(length, dtype=jnp.int32)
    opened = (offsets[:, None] <= position[None, :]).astype(jnp.int32)
    return jnp.sum(opened, axis=0) - 1


def contract_rows(left, right):
    return lax.dot_general(
        left, right, (((0,), (0,)), ((), ())), preferred_element_type=jnp.float32
    )


def contract_cols(left, right):
    return lax.dot_general(
        left, right, (((1,), (1,)), ((), ())), preferred_element_type=jnp.float32
    )


def on_device(byte_states, patch_start, queries, grad_out, w_kv):
    states = byte_states[0]
    all_offsets = patch_start[0]
    cotangent = grad_out[0]
    byte_count = states.shape[0]
    shard_total = all_offsets.shape[0]
    slot_count = all_offsets.shape[1]
    slot_total = shard_total * slot_count
    shard = lax.axis_index(BYTE)
    offsets = lax.dynamic_index_in_dim(all_offsets, shard, 0, keepdims=False)
    head_count = cotangent.shape[1] // HS
    shared_heads = w_kv.shape[2] // HS
    group_size = head_count // shared_heads
    factor = 1.0 / math.sqrt(HS)
    segments = segment_of(offsets, byte_count)
    slot_range = jnp.arange(slot_count, dtype=jnp.int32)
    members = slot_range[:, None] == segments[None, :]
    counts = jnp.maximum(jnp.sum(members.astype(jnp.float32), axis=1), 1.0)
    summed = jnp.dot(members.astype(jnp.bfloat16), states, preferred_element_type=jnp.float32)
    pooled_part = (summed / counts[:, None]).astype(jnp.bfloat16)
    usable = all_offsets.reshape(slot_total) < byte_count
    live = lax.dynamic_slice_in_dim(usable, shard * slot_count, slot_count, 0)
    core = lax.axis_index("dp")
    own = lax.dynamic_index_in_dim(w_kv, core, 0, keepdims=False)
    rows = copy_for_each(own, BYTE).reshape(-1, own.shape[1])
    pair_full = copy_for_each(rows, "dp")
    pooled = gathered_copies(pooled_part, "glob", 1)
    key_rows = jnp.dot(pooled, pair_full[0], preferred_element_type=jnp.float32).astype(
        jnp.bfloat16
    )
    value_rows = jnp.dot(pooled, pair_full[1], preferred_element_type=jnp.float32).astype(
        jnp.bfloat16
    )
    both_rows = jnp.concatenate([key_rows, value_rows], axis=1)
    both_all = copy_for_each(both_rows, BYTE).reshape(slot_total, both_rows.shape[1])
    key_all, value_all = jnp.split(both_all, 2, axis=1)
    block_len = math.gcd(slot_total, 1024)
    block_total = slot_total // block_len
    key_blocks = key_all.reshape(block_total, block_len, shared_heads, HS)
    value_blocks = value_all.reshape(block_total, block_len, shared_heads, HS)
    id_blocks = jnp.arange(slot_total, dtype=jnp.int32).reshape(block_total, block_len)
    usable_blocks = usable.reshape(block_total, block_len)
    query_heads = queries[0].reshape(slot_count, shared_heads, group_size, HS)
    query_ids = shard * slot_count + slot_range
    live_rows = live.astype(jnp.bfloat16)[:, None, None, None]
    masked_grad = cotangent.reshape(slot_count, shared_heads, group_size, HS) * live_rows

    def scores_of(key_block, id_block, usable_block):
        scores = (
            jnp.einsum("qcgd,kcd->cgqk", query_heads, key_block, preferred_element_type=jnp.float32)
            * factor
        )
        visible = (id_block[None, :] <= query_ids[:, None]) & usable_block[None, :]
        return (jnp.where(visible, scores, -1e30), visible)

    def first_pass(carried, blocks):
        highest, totals = carried
        key_block, id_block, usable_block = blocks
        masked, visible = scores_of(key_block, id_block, usable_block)
        newest = jnp.maximum(highest, jnp.max(masked, axis=-1))
        raised = jnp.where(visible, jnp.exp(masked - newest[..., None]), 0.0)
        totals = totals * jnp.exp(highest - newest) + jnp.sum(raised, axis=-1)
        return ((newest, totals), None)

    start_high = jnp.full((shared_heads, group_size, slot_count), -1e30, jnp.float32)
    (highest, totals), unused = lax.scan(
        first_pass, (start_high, jnp.zeros_like(start_high)), (key_blocks, id_blocks, usable_blocks)
    )
    totals = jnp.maximum(totals, 1.0)

    def attention_of(masked, visible):
        raised = jnp.where(visible, jnp.exp(masked - highest[..., None]), 0.0)
        return raised / totals[..., None]

    def second_pass(mixed, blocks):
        key_block, value_block, id_block, usable_block = blocks
        masked, visible = scores_of(key_block, id_block, usable_block)
        shortened = attention_of(masked, visible).astype(jnp.bfloat16)
        return (
            mixed
            + jnp.einsum(
                "cgqk,kcd->qcgd", shortened, value_block, preferred_element_type=jnp.float32
            ),
            None,
        )

    zero_heads = jnp.zeros((slot_count, shared_heads, group_size, HS), jnp.float32)
    all_blocks = (key_blocks, value_blocks, id_blocks, usable_blocks)
    mixed, unused = lax.scan(second_pass, zero_heads, all_blocks)
    attended = (mixed * live.astype(jnp.float32)[:, None, None, None]).astype(jnp.bfloat16)
    attended = attended.reshape(1, slot_count, head_count * HS)
    row_dots = jnp.einsum("qcgd,qcgd->cgq", masked_grad.astype(jnp.float32), mixed)

    def third_pass(query_acc, blocks):
        key_block, value_block, id_block, usable_block = blocks
        masked, visible = scores_of(key_block, id_block, usable_block)
        attention = attention_of(masked, visible)
        shortened = attention.astype(jnp.bfloat16)
        prob_grad = jnp.einsum(
            "qcgd,kcd->cgqk", masked_grad, value_block, preferred_element_type=jnp.float32
        )
        score_grad = (attention * (prob_grad - row_dots[..., None]) * factor).astype(jnp.bfloat16)
        query_acc = query_acc + jnp.einsum(
            "cgqk,kcd->qcgd", score_grad, key_block, preferred_element_type=jnp.float32
        )
        key_part = jnp.einsum(
            "cgqk,qcgd->kcd", score_grad, query_heads, preferred_element_type=jnp.float32
        )
        value_part = jnp.einsum(
            "cgqk,qcgd->kcd", shortened, masked_grad, preferred_element_type=jnp.float32
        )
        return (query_acc, (key_part, value_part))

    query_acc, (key_parts, value_parts) = lax.scan(third_pass, zero_heads, all_blocks)
    query_grad = query_acc.astype(jnp.bfloat16).reshape(1, slot_count, head_count * HS)
    key_terms = key_parts.reshape(slot_total, shared_heads * HS)
    value_terms = value_parts.reshape(slot_total, shared_heads * HS)
    key_sum, value_sum = sent_together_2(
        (key_terms.astype(jnp.bfloat16), value_terms.astype(jnp.bfloat16)), BYTE, 0, 1
    )
    key_grad = key_sum.astype(jnp.bfloat16)
    value_grad = value_sum.astype(jnp.bfloat16)
    patch_part = contract_cols(key_grad, pair_full[0]) + contract_cols(value_grad, pair_full[1])
    patch_grad = summed_on_arrival(patch_part.astype(jnp.bfloat16), "glob", 1).astype(jnp.bfloat16)
    pool_grad = patch_grad.astype(jnp.float32) / counts[:, None]
    byte_grad = jnp.take(pool_grad, segments, axis=0).astype(jnp.bfloat16)[None]
    pair_part = jnp.stack([contract_rows(pooled, key_grad), contract_rows(pooled, value_grad)])
    one_sum = summed_on_arrival(pair_part.astype(jnp.bfloat16), "dp", 0)[0]
    one_sum = summed_on_arrival(one_sum.astype(jnp.bfloat16), BYTE, 0)
    pair_grad = copy_for_each(one_sum, "dp")
    return (attended, query_grad, byte_grad, pair_grad)


def solution(mesh):
    torus = Mesh(
        mesh.devices.reshape(mesh.shape["dp"], mesh.shape["glob"], 8, 4),
        ("dp", "glob", "byte_0", "byte_1"),
    )
    in_specs = (
        P("dp", BYTE, "glob"),
        P("dp", None, None),
        P("dp", BYTE, "glob"),
        P("dp", BYTE, "glob"),
        P(None, BYTE, "glob"),
    )
    out_specs = (
        P("dp", BYTE, "glob"),
        P("dp", BYTE, "glob"),
        P("dp", BYTE, "glob"),
        P(None, BYTE, "glob"),
    )
    return jax.shard_map(
        on_device, mesh=torus, in_specs=in_specs, out_specs=out_specs, check_vma=False
    )
```

```python
import functools
import math

import jax
import jax.numpy as jnp
from jax import lax
from jax.experimental import pallas as pl
from jax.experimental.pallas import tpu as pltpu
from jax.sharding import Mesh
from jax.sharding import PartitionSpec as P

HS = 128
BYTE = ("byte_0", "byte_1")
CROSS = ("glob", "byte_1")
BF = jnp.bfloat16
F32 = jnp.float32


def exchange(value, axes):
    return lax.all_to_all(value, axes, split_axis=0, concat_axis=0, tiled=True)


def dot(left, right, over):
    return lax.dot_general(left, right, ((over[0], over[1]), ((), ())), preferred_element_type=F32)


def rows_by_cols(left, right):
    return dot(left, right, ((1,), (0,)))


def rows_by_rows(left, right):
    return dot(left, right, ((1,), (1,)))


def cols_by_cols(left, right):
    return dot(left, right, ((0,), (0,)))


def call(body, outs, *operands, name):
    specs = [pl.BlockSpec(memory_space=pltpu.SMEM)]
    specs += [pl.BlockSpec(memory_space=pltpu.VMEM) for _ in operands[1:]]
    return pl.pallas_call(
        body,
        out_shape=outs,
        in_specs=specs,
        out_specs=jax.tree.map(lambda _: pl.BlockSpec(memory_space=pltpu.VMEM), outs),
        compiler_params=pltpu.CompilerParams(vmem_limit_bytes=16 * 2**20),
        name=name,
    )(*operands)


def shape(dims, dtype=BF):
    return jax.ShapeDtypeStruct(dims, dtype)


def members_of(starts_ref, shard, byte_count):
    slot_count = starts_ref.shape[1]
    row = starts_ref[pl.ds(shard, 1), :]
    position = lax.broadcasted_iota(jnp.int32, (byte_count, slot_count), 0)
    slot = lax.broadcasted_iota(jnp.int32, (byte_count, slot_count), 1)
    segment = jnp.sum((row <= position).astype(jnp.int32), axis=1, keepdims=True) - 1
    return (segment == slot).astype(F32).astype(BF)


def counts_of(members):
    ones = jnp.ones((members.shape[0], HS), BF)
    return jnp.maximum(cols_by_cols(members, ones), 1.0)[:, :1]


def pool_body(place_ref, starts_ref, states_ref, out_ref):
    members = members_of(starts_ref, place_ref[0], states_ref.shape[0])
    summed = cols_by_cols(members, states_ref[...])
    pooled = (summed / counts_of(members)).astype(BF)
    globs, xs = out_ref.shape[:2]
    halves = out_ref.shape[3] // HS
    for x in range(xs):
        for half in range(halves):
            at = (half * xs + x) * HS
            for y in range(globs):
                out_ref[y, x, :, half * HS : (half + 1) * HS] = pooled[:, at : at + HS]


def project_body(place_ref, pooled_ref, pair_ref, out_ref):
    globs, xs, slots, width = pooled_ref.shape
    copies = out_ref.shape[0]
    for which in range(2):
        total = None
        for y in range(globs):
            left = pooled_ref[y].reshape(xs * slots, width)
            for half in range(width // HS):
                part = rows_by_cols(
                    left[:, half * HS : (half + 1) * HS], pair_ref[y * (width // HS) + half, which]
                )
                total = part if total is None else total + part
        rounded = total.astype(BF)
        for copy in range(copies):
            out_ref[copy, :, which * HS : (which + 1) * HS] = rounded


def gathered_sum(ref):
    total = ref[0].astype(F32)
    for at in range(1, ref.shape[0]):
        total = total + ref[at].astype(F32)
    return total


def share_body(place_ref, parts_ref, out_ref):
    total = gathered_sum(parts_ref).astype(out_ref.dtype)
    for copy in range(out_ref.shape[0]):
        out_ref[copy] = total


def attend_body(
    place_ref, starts_ref, query_ref, grad_ref, both_ref, attended_ref, query_grad_ref, both_grad_ref,
    *, byte_count
):
    shard = place_ref[0]
    shard_total, slot_count = starts_ref.shape
    slot_total = shard_total * slot_count
    heads = query_ref.shape[1] // HS
    factor = 1.0 / math.sqrt(HS)
    used = jnp.sum((starts_ref[...] < byte_count).astype(jnp.int32), axis=1, keepdims=True)
    ids = lax.broadcasted_iota(jnp.int32, (shard_total, slot_total), 1)
    shards = lax.broadcasted_iota(jnp.int32, (shard_total, slot_total), 0)
    inside = ids - shards * slot_count
    usable = jnp.max(
        ((inside >= 0) & (inside < used)).astype(F32), axis=0, keepdims=True
    )
    mine = lax.broadcasted_iota(jnp.int32, (shard_total, 1), 0) == shard
    own_used = jnp.sum(jnp.where(mine, used, 0), axis=0, keepdims=True)
    live = (lax.broadcasted_iota(jnp.int32, (slot_count, 1), 0) < own_used).astype(F32)
    rows = lax.broadcasted_iota(jnp.int32, (slot_count, slot_total), 0) + shard * slot_count
    cols = lax.broadcasted_iota(jnp.int32, (slot_count, slot_total), 1)
    visible = (cols <= rows) & (usable > 0.0)
    keys = both_ref[:, :HS]
    values = both_ref[:, HS:]
    queries, grads, shorts, score_grads = [], [], [], []
    for head in range(heads):
        at = slice(head * HS, (head + 1) * HS)
        query = query_ref[:, at]
        grad = (grad_ref[:, at].astype(F32) * live).astype(BF)
        scores = jnp.where(visible, rows_by_rows(query, keys) * factor, -1e30)
        highest = jnp.max(scores, axis=1, keepdims=True)
        raised = jnp.where(visible, jnp.exp(scores - highest), 0.0)
        total = jnp.maximum(jnp.sum(raised, axis=1, keepdims=True), 1.0)
        attention = raised / total
        short = attention.astype(BF)
        mixed = rows_by_cols(short, values)
        attended_ref[:, at] = (mixed * live).astype(BF)
        dots = jnp.sum(grad.astype(F32) * mixed, axis=1, keepdims=True)
        prob_grad = rows_by_rows(grad, values)
        score_grad = (attention * (prob_grad - dots) * factor).astype(BF)
        query_grad_ref[:, at] = rows_by_cols(score_grad, keys).astype(BF)
        queries.append(query)
        grads.append(grad)
        shorts.append(short)
        score_grads.append(score_grad)
    queries = jnp.concatenate(queries, axis=0)
    grads = jnp.concatenate(grads, axis=0)
    both_grad_ref[:, :HS] = cols_by_cols(jnp.concatenate(score_grads, axis=0), queries).astype(BF)
    both_grad_ref[:, HS:] = cols_by_cols(jnp.concatenate(shorts, axis=0), grads).astype(BF)


def spread_body(place_ref, parts_ref, pooled_ref, pair_ref, patch_ref, weight_ref):
    both = gathered_sum(parts_ref).astype(BF)
    globs, xs, slots, width = pooled_ref.shape
    halves = width // HS
    for y in range(globs):
        left = pooled_ref[y].reshape(xs * slots, width)
        for half in range(halves):
            block = y * halves + half
            total = rows_by_rows(both[:, :HS], pair_ref[block, 0])
            total = total + rows_by_rows(both[:, HS:], pair_ref[block, 1])
            patch_ref[y, :, :, half * HS : (half + 1) * HS] = total.astype(BF).reshape(xs, slots, HS)
            grad = cols_by_cols(left[:, half * HS : (half + 1) * HS], both).astype(BF)
            weight_ref[0, block] = grad[:, :HS]
            weight_ref[1, block] = grad[:, HS:]


def byte_body(place_ref, starts_ref, parts_ref, out_ref):
    members = members_of(starts_ref, place_ref[0], out_ref.shape[0])
    counts = counts_of(members)
    globs, xs, slots, width = parts_ref.shape
    for x in range(xs):
        total = parts_ref[0, x].astype(F32)
        for y in range(1, globs):
            total = total + parts_ref[y, x].astype(F32)
        shared = (total.astype(BF).astype(F32) / counts).astype(BF)
        for half in range(width // HS):
            at = (half * xs + x) * HS
            out_ref[:, at : at + HS] = rows_by_cols(
                members, shared[:, half * HS : (half + 1) * HS]
            ).astype(BF)


def on_device(byte_states, patch_start, queries, grad_out, w_kv):
    states = byte_states[0]
    starts = patch_start[0]
    byte_count, width = states.shape
    shard_total, slot_count = starts.shape
    slot_total = shard_total * slot_count
    globs = lax.axis_size("glob")
    depth = lax.axis_size("byte_0")
    across = lax.axis_size("byte_1")
    block = slot_total // depth
    both = 2 * HS
    halves = width // (across * HS)
    place = jnp.reshape(lax.axis_index(BYTE), (1,)).astype(jnp.int32)

    pair = exchange(jnp.broadcast_to(w_kv, (depth, *w_kv.shape)), "byte_0")
    send = call(
        pool_body, shape((globs, across, slot_count, halves * HS)), place, starts, states, name="pool"
    )
    pooled = exchange(send.reshape(globs * across, slot_count, halves * HS), CROSS)
    pooled = pooled.reshape(globs, across, slot_count, halves * HS)
    send = call(project_body, shape((across, block, both)), place, pooled, pair, name="project")
    parts = exchange(send, "byte_1")
    send = call(share_body, shape((depth, block, both)), place, parts, name="share")
    key_value = exchange(send, "byte_0").reshape(slot_total, both)
    rows = queries.shape[1:]
    attended, query_grad, send = call(
        functools.partial(attend_body, byte_count=byte_count),
        (shape(rows), shape(rows), shape((slot_total, both))),
        place, starts, queries[0], grad_out[0], key_value,
        name="attend",
    )
    parts = exchange(send.reshape(depth, block, both), "byte_0")
    send = call(share_body, shape((across, block, both)), place, parts, name="share_grad")
    parts = exchange(send, "byte_1")
    patch_send, weight_send = call(
        spread_body,
        (shape((globs, across, slot_count, halves * HS)), shape((2, depth, HS, HS))),
        place, parts, pooled, pair,
        name="spread",
    )
    parts = exchange(patch_send.reshape(globs * across, slot_count, halves * HS), CROSS)
    parts = parts.reshape(globs, across, slot_count, halves * HS)
    weight_parts = exchange(weight_send, "dp")
    byte_grad = call(byte_body, shape((byte_count, width)), place, starts, parts, name="bytes")
    send = call(share_body, shape((1, depth, HS, HS)), place, weight_parts, name="sum_dp")
    weight_parts = exchange(send[0], "byte_0")
    send = call(share_body, shape((2, HS, HS), F32), place, weight_parts, name="sum_byte")
    pair_grad = exchange(send, "dp")
    return (attended[None], query_grad[None], byte_grad[None], pair_grad)


def solution(mesh):
    torus = Mesh(
        mesh.devices.reshape(mesh.shape["dp"], mesh.shape["glob"], 8, 4),
        ("dp", "glob", "byte_0", "byte_1"),
    )
    in_specs = (
        P("dp", BYTE, "glob"),
        P("dp", None, None),
        P("dp", BYTE, "glob"),
        P("dp", BYTE, "glob"),
        P(None, BYTE, "glob"),
    )
    out_specs = (
        P("dp", BYTE, "glob"),
        P("dp", BYTE, "glob"),
        P("dp", BYTE, "glob"),
        P(None, BYTE, "glob"),
    )
    return jax.shard_map(
        on_device, mesh=torus, in_specs=in_specs, out_specs=out_specs, check_vma=False
    )
```

```python
import functools
import math

import jax
import jax.numpy as jnp
from jax import lax
from jax.experimental import pallas as pl
from jax.experimental.pallas import tpu as pltpu
from jax.sharding import Mesh
from jax.sharding import PartitionSpec as P

HS = 128
BYTE = ("byte_0", "byte_1")
CROSS = ("dp", "glob", "byte_1")
NEAR = ("dp", "byte_1")
BF = jnp.bfloat16
F32 = jnp.float32


def exchange(value, axes):
    return lax.all_to_all(value, axes, split_axis=0, concat_axis=0, tiled=True)


def dot(left, right, over):
    return lax.dot_general(left, right, ((over[0], over[1]), ((), ())), preferred_element_type=F32)


def rows_by_cols(left, right):
    return dot(left, right, ((1,), (0,)))


def rows_by_rows(left, right):
    return dot(left, right, ((1,), (1,)))


def cols_by_cols(left, right):
    return dot(left, right, ((0,), (0,)))


def call(body, outs, *operands, name):
    specs = [pl.BlockSpec(memory_space=pltpu.SMEM)]
    specs += [pl.BlockSpec(memory_space=pltpu.VMEM) for _ in operands[1:]]
    return pl.pallas_call(
        body,
        out_shape=outs,
        in_specs=specs,
        out_specs=jax.tree.map(lambda _: pl.BlockSpec(memory_space=pltpu.VMEM), outs),
        compiler_params=pltpu.CompilerParams(vmem_limit_bytes=16 * 2**20),
        name=name,
    )(*operands)


def shape(dims, dtype=BF):
    return jax.ShapeDtypeStruct(dims, dtype)


def members_of(starts_ref, shard, byte_count):
    slot_count = starts_ref.shape[1]
    row = starts_ref[pl.ds(shard, 1), :]
    position = lax.broadcasted_iota(jnp.int32, (byte_count, slot_count), 0)
    slot = lax.broadcasted_iota(jnp.int32, (byte_count, slot_count), 1)
    segment = jnp.sum((row <= position).astype(jnp.int32), axis=1, keepdims=True) - 1
    return (segment == slot).astype(F32).astype(BF)


def counts_of(members):
    ones = jnp.ones((members.shape[0], HS), BF)
    return jnp.maximum(cols_by_cols(members, ones), 1.0)[:, :1]


def first_half(shape):
    return lax.broadcasted_iota(jnp.int32, shape, 1) < HS // 2


def halves_paired(low, high, first):
    select = first_half(low.shape)
    if first:
        return jnp.where(select, low, pltpu.roll(high, HS // 2, 1))
    return jnp.where(select, pltpu.roll(low, HS // 2, 1), high)


def pool_body(place_ref, starts_ref, states_ref, out_ref):
    members = members_of(starts_ref, place_ref[0], states_ref.shape[0])
    summed = cols_by_cols(members, states_ref[...])
    pooled = summed / counts_of(members)
    cores, globs, xs = out_ref.shape[:3]
    for x in range(xs):
        low = pooled[:, x * HS : (x + 1) * HS]
        high = pooled[:, (xs + x) * HS : (xs + x + 1) * HS]
        for core in range(cores):
            piece = halves_paired(low, high, core == 0).astype(BF)
            for y in range(globs):
                out_ref[core, y, x] = piece


def copy_body(place_ref, pair_ref, out_ref):
    depth, rows = out_ref.shape[:2]
    at = pl.multiple_of(place_ref[1] * rows, rows)
    for which in range(2):
        piece = pair_ref[which, pl.ds(at, rows), :]
        for z in range(depth):
            out_ref[z, :, which * HS : (which + 1) * HS] = piece


def features_of(pooled_ref, core):
    globs, xs, slots = pooled_ref.shape[1:4]
    pieces = [pooled_ref[core, y].reshape(xs * slots, HS) for y in range(globs)]
    return jnp.concatenate(pieces, axis=1)


def weights_of(pair_ref):
    depth, rows, cols = pair_ref.shape
    return pair_ref[...].reshape(depth * rows, cols)


def project_body(place_ref, pooled_ref, pair_ref, out_ref):
    weights = weights_of(pair_ref)
    for core in range(out_ref.shape[0]):
        rounded = rows_by_cols(features_of(pooled_ref, core), weights).astype(BF)
        for copy in range(out_ref.shape[1]):
            out_ref[core, copy] = rounded


def gathered_sum(ref):
    total = ref[0].astype(F32)
    for at in range(1, ref.shape[0]):
        total = total + ref[at].astype(F32)
    return total


def share_body(place_ref, parts_ref, out_ref):
    total = gathered_sum(parts_ref).astype(out_ref.dtype)
    for copy in range(out_ref.shape[0]):
        out_ref[copy] = total


def attend_body(
    place_ref, starts_ref, query_ref, grad_ref, both_ref, attended_ref, query_grad_ref, both_grad_ref,
    *, byte_count
):
    shard = place_ref[0]
    shard_total, slot_count = starts_ref.shape
    slot_total = shard_total * slot_count
    heads = query_ref.shape[1] // HS
    factor = 1.0 / math.sqrt(HS)
    used = jnp.sum((starts_ref[...] < byte_count).astype(jnp.int32), axis=1, keepdims=True)
    ids = lax.broadcasted_iota(jnp.int32, (shard_total, slot_total), 1)
    shards = lax.broadcasted_iota(jnp.int32, (shard_total, slot_total), 0)
    inside = ids - shards * slot_count
    usable = jnp.max(
        ((inside >= 0) & (inside < used)).astype(F32), axis=0, keepdims=True
    )
    mine = lax.broadcasted_iota(jnp.int32, (shard_total, 1), 0) == shard
    own_used = jnp.sum(jnp.where(mine, used, 0), axis=0, keepdims=True)
    live = (lax.broadcasted_iota(jnp.int32, (slot_count, 1), 0) < own_used).astype(F32)
    rows = lax.broadcasted_iota(jnp.int32, (slot_count, slot_total), 0) + shard * slot_count
    cols = lax.broadcasted_iota(jnp.int32, (slot_count, slot_total), 1)
    visible = (cols <= rows) & (usable > 0.0)
    keys = both_ref[:, :HS]
    values = both_ref[:, HS:]
    queries, grads, shorts, score_grads = [], [], [], []
    for head in range(heads):
        at = slice(head * HS, (head + 1) * HS)
        query = query_ref[:, at]
        grad = (grad_ref[:, at].astype(F32) * live).astype(BF)
        scores = jnp.where(visible, rows_by_rows(query, keys) * factor, -1e30)
        highest = jnp.max(scores, axis=1, keepdims=True)
        raised = jnp.where(visible, jnp.exp(scores - highest), 0.0)
        total = jnp.maximum(jnp.sum(raised, axis=1, keepdims=True), 1.0)
        attention = raised / total
        short = attention.astype(BF)
        mixed = rows_by_cols(short, values)
        attended_ref[:, at] = (mixed * live).astype(BF)
        dots = jnp.sum(grad.astype(F32) * mixed, axis=1, keepdims=True)
        prob_grad = rows_by_rows(grad, values)
        score_grad = (attention * (prob_grad - dots) * factor).astype(BF)
        query_grad_ref[:, at] = rows_by_cols(score_grad, keys).astype(BF)
        queries.append(query)
        grads.append(grad)
        shorts.append(short)
        score_grads.append(score_grad)
    queries = jnp.concatenate(queries, axis=0)
    grads = jnp.concatenate(grads, axis=0)
    both_grad_ref[:, :HS] = cols_by_cols(jnp.concatenate(score_grads, axis=0), queries).astype(BF)
    both_grad_ref[:, HS:] = cols_by_cols(jnp.concatenate(shorts, axis=0), grads).astype(BF)


def spread_body(place_ref, parts_ref, pooled_ref, pair_ref, patch_ref, weight_ref):
    weights = weights_of(pair_ref)
    cores, globs, xs, slots = pooled_ref.shape[:4]
    grads = []
    for core in range(cores):
        total = parts_ref[core * xs].astype(F32)
        for x in range(1, xs):
            total = total + parts_ref[core * xs + x].astype(F32)
        grad = total.astype(BF)
        patch = rows_by_rows(grad, weights).astype(BF)
        for y in range(globs):
            patch_ref[core, y] = patch[:, y * HS : (y + 1) * HS].reshape(xs, slots, HS)
        grads.append(grad)
    features = jnp.concatenate([features_of(pooled_ref, core) for core in range(cores)], axis=0)
    weight = cols_by_cols(features, jnp.concatenate(grads, axis=0)).astype(BF)
    weight_ref[...] = weight.reshape(weight_ref.shape)


def byte_body(place_ref, starts_ref, parts_ref, out_ref):
    members = members_of(starts_ref, place_ref[0], out_ref.shape[0])
    counts = counts_of(members)
    cores, globs, xs = parts_ref.shape[:3]
    for x in range(xs):
        totals = []
        for core in range(cores):
            total = parts_ref[core, 0, x].astype(F32)
            for y in range(1, globs):
                total = total + parts_ref[core, y, x].astype(F32)
            totals.append(total.astype(BF).astype(F32) / counts)
        for half in range(2):
            shared = halves_paired(*totals, half == 0).astype(BF)
            at = (half * xs + x) * HS
            out_ref[:, at : at + HS] = rows_by_cols(members, shared).astype(BF)


def total_body(place_ref, parts_ref, out_ref):
    total = gathered_sum(parts_ref)
    for copy in range(out_ref.shape[0]):
        for which in range(2):
            out_ref[copy, which] = total[:, which * HS : (which + 1) * HS]


def on_device(byte_states, patch_start, queries, grad_out, w_kv):
    states = byte_states[0]
    starts = patch_start[0]
    byte_count, width = states.shape
    shard_total, slot_count = starts.shape
    slot_total = shard_total * slot_count
    cores = lax.axis_size("dp")
    globs = lax.axis_size("glob")
    depth = lax.axis_size("byte_0")
    across = lax.axis_size("byte_1")
    block = slot_total // depth
    both = 2 * HS
    half = HS // cores
    pieces = (cores, globs, across, slot_count, HS)
    place = jnp.stack([lax.axis_index(BYTE), lax.axis_index("dp")]).astype(jnp.int32)

    send = call(copy_body, shape((depth, half, both)), place, w_kv, name="copies")
    pair = exchange(send, "byte_0")
    send = call(pool_body, shape(pieces), place, starts, states, name="pool")
    pooled = exchange(send.reshape(-1, slot_count, HS), CROSS).reshape(pieces)
    send = call(project_body, shape((cores, across, block, both)), place, pooled, pair, name="project")
    parts = exchange(send.reshape(-1, block, both), NEAR)
    send = call(share_body, shape((depth, block, both)), place, parts, name="share")
    key_value = exchange(send, "byte_0").reshape(slot_total, both)
    rows = queries.shape[1:]
    attended, query_grad, send = call(
        functools.partial(attend_body, byte_count=byte_count),
        (shape(rows), shape(rows), shape((slot_total, both))),
        place, starts, queries[0], grad_out[0], key_value,
        name="attend",
    )
    parts = exchange(send.reshape(depth, block, both), "byte_0")
    send = call(share_body, shape((cores * across, block, both)), place, parts, name="share_grad")
    parts = exchange(send, NEAR)
    patch_send, weight_send = call(
        spread_body, (shape(pieces), shape((depth, half, both))), place, parts, pooled, pair,
        name="spread",
    )
    parts = exchange(patch_send.reshape(-1, slot_count, HS), CROSS).reshape(pieces)
    byte_grad = call(byte_body, shape((byte_count, width)), place, starts, parts, name="bytes")
    weight_parts = exchange(weight_send, "byte_0")
    send = call(total_body, shape((cores, 2, half, HS), F32), place, weight_parts, name="total")
    pair_grad = exchange(send, "dp").transpose(1, 0, 2, 3).reshape(w_kv.shape)
    return (attended[None], query_grad[None], byte_grad[None], pair_grad)


def solution(mesh):
    torus = Mesh(
        mesh.devices.reshape(mesh.shape["dp"], mesh.shape["glob"], 8, 4),
        ("dp", "glob", "byte_0", "byte_1"),
    )
    in_specs = (
        P("dp", BYTE, "glob"),
        P("dp", None, None),
        P("dp", BYTE, "glob"),
        P("dp", BYTE, "glob"),
        P(None, BYTE, "glob"),
    )
    out_specs = (
        P("dp", BYTE, "glob"),
        P("dp", BYTE, "glob"),
        P("dp", BYTE, "glob"),
        P(None, BYTE, "glob"),
    )
    return jax.shard_map(
        on_device, mesh=torus, in_specs=in_specs, out_specs=out_specs, check_vma=False
    )
```

```python
import functools
import math

import jax
import jax.numpy as jnp
from jax import lax
from jax.experimental import pallas as pl
from jax.experimental.pallas import tpu as pltpu
from jax.sharding import Mesh
from jax.sharding import PartitionSpec as P

HS = 128
BYTE = ("byte_0", "byte_1")
CROSS = ("glob", "byte_1")
BF = jnp.bfloat16
F32 = jnp.float32


def exchange(value, axes):
    return lax.all_to_all(value, axes, split_axis=0, concat_axis=0, tiled=True)


def dot(left, right, over):
    return lax.dot_general(left, right, ((over[0], over[1]), ((), ())), preferred_element_type=F32)


def rows_by_cols(left, right):
    return dot(left, right, ((1,), (0,)))


def rows_by_rows(left, right):
    return dot(left, right, ((1,), (1,)))


def cols_by_cols(left, right):
    return dot(left, right, ((0,), (0,)))


def call(body, outs, *operands, name):
    specs = [pl.BlockSpec(memory_space=pltpu.VMEM) for _ in operands]
    return pl.pallas_call(
        body,
        out_shape=outs,
        in_specs=specs,
        out_specs=jax.tree.map(lambda _: pl.BlockSpec(memory_space=pltpu.VMEM), outs),
        compiler_params=pltpu.CompilerParams(vmem_limit_bytes=16 * 2**20),
        name=name,
    )(*operands)


def shape(dims, dtype=BF):
    return jax.ShapeDtypeStruct(dims, dtype)


def members_of(starts_ref, shard, byte_count):
    slot_count = starts_ref.shape[1]
    row = starts_ref[pl.ds(shard, 1), :]
    position = lax.broadcasted_iota(jnp.int32, (byte_count, slot_count), 0)
    slot = lax.broadcasted_iota(jnp.int32, (byte_count, slot_count), 1)
    segment = jnp.sum((row <= position).astype(jnp.int32), axis=1, keepdims=True) - 1
    return (segment == slot).astype(F32).astype(BF)


def counts_of(members):
    ones = jnp.ones((members.shape[0], HS), BF)
    return jnp.maximum(cols_by_cols(members, ones), 1.0)[:, :1]


def pool_body(starts_ref, states_ref, out_ref):
    members = members_of(starts_ref, lax.axis_index(BYTE), states_ref.shape[0])
    summed = cols_by_cols(members, states_ref[...])
    pooled = (summed / counts_of(members)).astype(BF)
    globs, xs = out_ref.shape[:2]
    halves = out_ref.shape[3] // HS
    for x in range(xs):
        for half in range(halves):
            at = (half * xs + x) * HS
            for y in range(globs):
                out_ref[y, x, :, half * HS : (half + 1) * HS] = pooled[:, at : at + HS]


def copy_body(pair_ref, out_ref):
    first = lax.axis_index("dp") == 0
    piece = jnp.where(first, pair_ref[0], pair_ref[1])
    for z in range(out_ref.shape[0]):
        out_ref[z] = piece


def features_of(pooled_ref):
    globs, xs, slots, width = pooled_ref.shape
    return jnp.concatenate([pooled_ref[y].reshape(xs * slots, width) for y in range(globs)], axis=1)


def pair_of(own_ref, other_ref):
    flat = (own_ref.shape[0] * own_ref.shape[1], own_ref.shape[2])
    return own_ref[...].reshape(flat), other_ref[...].reshape(flat)


def ordered(own, other):
    first = lax.axis_index("dp") == 0
    return jnp.where(first, own, other), jnp.where(first, other, own)


def project_body(pooled_ref, own_ref, other_ref, out_ref):
    left = features_of(pooled_ref)
    parts = [rows_by_cols(left, m).astype(BF) for m in ordered(*pair_of(own_ref, other_ref))]
    for copy in range(out_ref.shape[0]):
        for which in range(2):
            out_ref[copy, :, which * HS : (which + 1) * HS] = parts[which]


def gathered_sum(ref):
    total = ref[0].astype(F32)
    for at in range(1, ref.shape[0]):
        total = total + ref[at].astype(F32)
    return total


def share_body(parts_ref, out_ref):
    total = gathered_sum(parts_ref).astype(out_ref.dtype)
    for copy in range(out_ref.shape[0]):
        out_ref[copy] = total


def stacked(value, heads):
    return jnp.concatenate([value[:, h * HS : (h + 1) * HS] for h in range(heads)], axis=0)


def side_by_side(value, heads):
    rows = value.shape[0] // heads
    return jnp.concatenate([value[h * rows : (h + 1) * rows] for h in range(heads)], axis=1)


def attend_body(
    starts_ref, query_ref, grad_ref, both_ref, attended_ref, query_grad_ref, both_grad_ref,
    *, byte_count
):
    shard = lax.axis_index(BYTE)
    shard_total, slot_count = starts_ref.shape
    slot_total = shard_total * slot_count
    heads = query_ref.shape[1] // HS
    factor = 1.0 / math.sqrt(HS)
    used = jnp.sum((starts_ref[...] < byte_count).astype(jnp.int32), axis=1, keepdims=True)
    ids = lax.broadcasted_iota(jnp.int32, (shard_total, slot_total), 1)
    shards = lax.broadcasted_iota(jnp.int32, (shard_total, slot_total), 0)
    inside = ids - shards * slot_count
    usable = jnp.max(
        ((inside >= 0) & (inside < used)).astype(F32), axis=0, keepdims=True
    )
    mine = lax.broadcasted_iota(jnp.int32, (shard_total, 1), 0) == shard
    own_used = jnp.sum(jnp.where(mine, used, 0), axis=0, keepdims=True)
    live = (lax.broadcasted_iota(jnp.int32, (slot_count, 1), 0) < own_used).astype(F32)
    rows = lax.broadcasted_iota(jnp.int32, (slot_count, slot_total), 0) + shard * slot_count
    cols = lax.broadcasted_iota(jnp.int32, (slot_count, slot_total), 1)
    visible = (cols <= rows) & (usable > 0.0)
    keys = both_ref[:, :HS]
    values = both_ref[:, HS:]
    query = stacked(query_ref[...], heads)
    grad = stacked(grad_ref[...], heads)
    live_rows = jnp.concatenate([live] * heads, axis=0)
    seen = jnp.concatenate([visible.astype(F32)] * heads, axis=0) > 0.0
    grad = (grad.astype(F32) * live_rows).astype(BF)
    scores = jnp.where(seen, rows_by_rows(query, keys) * factor, -1e30)
    highest = jnp.max(scores, axis=1, keepdims=True)
    raised = jnp.where(seen, jnp.exp(scores - highest), 0.0)
    total = jnp.maximum(jnp.sum(raised, axis=1, keepdims=True), 1.0)
    attention = raised * (1.0 / total)
    short = attention.astype(BF)
    mixed = rows_by_cols(short, values)
    attended_ref[...] = side_by_side((mixed * live_rows).astype(BF), heads)
    dots = jnp.sum(grad.astype(F32) * mixed, axis=1, keepdims=True)
    prob_grad = rows_by_rows(grad, values)
    score_grad = (attention * ((prob_grad - dots) * factor)).astype(BF)
    query_grad_ref[...] = side_by_side(rows_by_cols(score_grad, keys).astype(BF), heads)
    both_grad_ref[:, :HS] = cols_by_cols(score_grad, query).astype(BF)
    both_grad_ref[:, HS:] = cols_by_cols(short, grad).astype(BF)


def spread_body(parts_ref, pooled_ref, own_ref, other_ref, patch_ref, keep_ref, give_ref):
    both = gathered_sum(parts_ref).astype(BF)
    globs, xs, slots, width = pooled_ref.shape
    weights = ordered(*pair_of(own_ref, other_ref))
    patch = rows_by_rows(both[:, :HS], weights[0]) + rows_by_rows(both[:, HS:], weights[1])
    patch = patch.astype(BF)
    for y in range(globs):
        patch_ref[y] = patch[:, y * width : (y + 1) * width].reshape(xs, slots, width)
    grad = cols_by_cols(features_of(pooled_ref), both)
    keep, give = ordered(grad[:, :HS].astype(BF), grad[:, HS:].astype(BF))
    keep_ref[...] = keep.reshape(keep_ref.shape)
    give_ref[...] = give.reshape(give_ref.shape)


def add_body(left_ref, right_ref, out_ref):
    out_ref[...] = (left_ref[...].astype(F32) + right_ref[...].astype(F32)).astype(BF)


def byte_body(starts_ref, parts_ref, out_ref):
    members = members_of(starts_ref, lax.axis_index(BYTE), out_ref.shape[0])
    counts = counts_of(members)
    globs, xs, slots, width = parts_ref.shape
    pieces = [None] * (xs * width // HS)
    for x in range(xs):
        total = parts_ref[0, x].astype(F32)
        for y in range(1, globs):
            total = total + parts_ref[y, x].astype(F32)
        shared = (total.astype(BF).astype(F32) / counts).astype(BF)
        for half in range(width // HS):
            pieces[half * xs + x] = shared[:, half * HS : (half + 1) * HS]
    out_ref[...] = rows_by_cols(members, jnp.concatenate(pieces, axis=1)).astype(BF)


def on_device(byte_states, patch_start, queries, grad_out, w_kv):
    states = byte_states[0]
    starts = patch_start[0]
    byte_count, width = states.shape
    shard_total, slot_count = starts.shape
    slot_total = shard_total * slot_count
    globs = lax.axis_size("glob")
    depth = lax.axis_size("byte_0")
    across = lax.axis_size("byte_1")
    block = slot_total // depth
    both = 2 * HS
    halves = width // (across * HS)

    swap = [(0, 1), (1, 0)]
    own = exchange(call(copy_body, shape((depth, HS, HS)), w_kv, name="copies"), "byte_0")
    other = lax.ppermute(own, "dp", swap)
    send = call(
        pool_body, shape((globs, across, slot_count, halves * HS)), starts, states, name="pool"
    )
    pooled = exchange(send.reshape(globs * across, slot_count, halves * HS), CROSS)
    pooled = pooled.reshape(globs, across, slot_count, halves * HS)
    send = call(project_body, shape((across, block, both)), pooled, own, other, name="project")
    parts = exchange(send, "byte_1")
    send = call(share_body, shape((depth, block, both)), parts, name="share")
    key_value = exchange(send, "byte_0").reshape(slot_total, both)
    rows = queries.shape[1:]
    attended, query_grad, send = call(
        functools.partial(attend_body, byte_count=byte_count),
        (shape(rows), shape(rows), shape((slot_total, both))),
        starts, queries[0], grad_out[0], key_value,
        name="attend",
    )
    parts = exchange(send.reshape(depth, block, both), "byte_0")
    send = call(share_body, shape((across, block, both)), parts, name="share_grad")
    parts = exchange(send, "byte_1")
    blocks = shape((depth, HS, HS))
    patch_send, keep, give = call(
        spread_body, (shape((globs, across, slot_count, halves * HS)), blocks, blocks),
        parts, pooled, own, other,
        name="spread",
    )
    given = lax.ppermute(give, "dp", swap)
    parts = exchange(patch_send.reshape(globs * across, slot_count, halves * HS), CROSS)
    parts = parts.reshape(globs, across, slot_count, halves * HS)
    byte_grad = call(byte_body, shape((byte_count, width)), starts, parts, name="bytes")
    send = call(add_body, blocks, keep, given, name="sum_dp")
    weight_parts = exchange(send, "byte_0")
    send = call(share_body, shape((2, HS, HS), F32), weight_parts, name="sum_byte")
    pair_grad = exchange(send, "dp")
    return (attended[None], query_grad[None], byte_grad[None], pair_grad)


def solution(mesh):
    torus = Mesh(
        mesh.devices.reshape(mesh.shape["dp"], mesh.shape["glob"], 8, 4),
        ("dp", "glob", "byte_0", "byte_1"),
    )
    in_specs = (
        P("dp", BYTE, "glob"),
        P("dp", None, None),
        P("dp", BYTE, "glob"),
        P("dp", BYTE, "glob"),
        P(None, BYTE, "glob"),
    )
    out_specs = (
        P("dp", BYTE, "glob"),
        P("dp", BYTE, "glob"),
        P("dp", BYTE, "glob"),
        P(None, BYTE, "glob"),
    )
    return jax.shard_map(
        on_device, mesh=torus, in_specs=in_specs, out_specs=out_specs, check_vma=False
    )
```

```python
import functools
import math

import jax
import jax.numpy as jnp
from jax import lax
from jax.experimental import pallas as pl
from jax.experimental.pallas import tpu as pltpu
from jax.sharding import Mesh
from jax.sharding import PartitionSpec as P


HS = 128
BYTE = ("byte_0", "byte_1")
CROSS = ("glob", "byte_1")
BF = jnp.bfloat16
F32 = jnp.float32


def exchange(value, axes):
    return lax.all_to_all(value, axes, split_axis=0, concat_axis=0, tiled=True)


def dot(left, right, over):
    return lax.dot_general(left, right, ((over[0], over[1]), ((), ())), preferred_element_type=F32)


def rows_by_cols(left, right):
    return dot(left, right, ((1,), (0,)))


def rows_by_rows(left, right):
    return dot(left, right, ((1,), (1,)))


def cols_by_cols(left, right):
    return dot(left, right, ((0,), (0,)))


def call(body, outs, *operands, name):
    specs = [pl.BlockSpec(memory_space=pltpu.VMEM) for _ in operands]
    return pl.pallas_call(
        body,
        out_shape=outs,
        in_specs=specs,
        out_specs=jax.tree.map(lambda _: pl.BlockSpec(memory_space=pltpu.VMEM), outs),
        compiler_params=pltpu.CompilerParams(vmem_limit_bytes=16 * 2**20),
        name=name,
    )(*operands)


def shape(dims, dtype=BF):
    return jax.ShapeDtypeStruct(dims, dtype)


def members_of(starts_ref, shard, byte_count):
    slot_count = starts_ref.shape[1]
    row = starts_ref[pl.ds(shard, 1), :]
    position = lax.broadcasted_iota(jnp.int32, (byte_count, slot_count), 0)
    slot = lax.broadcasted_iota(jnp.int32, (byte_count, slot_count), 1)
    segment = jnp.sum((row <= position).astype(jnp.int32), axis=1, keepdims=True) - 1
    return (segment == slot).astype(F32).astype(BF)


def counts_of(members):
    ones = jnp.ones((members.shape[0], HS), BF)
    return jnp.maximum(cols_by_cols(members, ones), 1.0)[:, :1]


def pool_body(starts_ref, states_ref, out_ref):
    members = members_of(starts_ref, lax.axis_index(BYTE), states_ref.shape[0])
    summed = cols_by_cols(members, states_ref[...])
    pooled = (summed / counts_of(members)).astype(BF)
    globs, xs = out_ref.shape[:2]
    for x in range(xs):
        for half in range(out_ref.shape[2]):
            at = (half * xs + x) * HS
            for y in range(globs):
                out_ref[y, x, half] = pooled[:, at : at + HS]


def partner(step):
    z = lax.bitwise_xor(lax.axis_index("byte_0"), step)
    return z // 2, lax.rem(z, 2)


def feature_block(pooled_ref, step):
    y, half = partner(step)
    return pooled_ref[y, :, half].reshape(-1, HS)


def project_body(pooled_ref, *refs):
    *pairs, out_ref = refs
    left = jnp.concatenate([feature_block(pooled_ref, k) for k in range(len(pairs))], axis=1)
    for which in range(2):
        weights = jnp.concatenate([pair[which] for pair in pairs], axis=0)
        part = rows_by_cols(left, weights).astype(BF)
        for copy in range(out_ref.shape[0]):
            out_ref[copy, :, which * HS : (which + 1) * HS] = part


def gathered_sum(ref):
    total = ref[0].astype(F32)
    for at in range(1, ref.shape[0]):
        total = total + ref[at].astype(F32)
    return total


def share_body(parts_ref, out_ref):
    total = gathered_sum(parts_ref).astype(out_ref.dtype)
    for copy in range(out_ref.shape[0]):
        out_ref[copy] = total


def stacked(value, heads):
    return jnp.concatenate([value[:, h * HS : (h + 1) * HS] for h in range(heads)], axis=0)


def side_by_side(value, heads):
    rows = value.shape[0] // heads
    return jnp.concatenate([value[h * rows : (h + 1) * rows] for h in range(heads)], axis=1)


def attend_body(
    starts_ref, query_ref, grad_ref, both_ref, attended_ref, query_grad_ref, both_grad_ref,
    *, byte_count
):
    shard = lax.axis_index(BYTE)
    shard_total, slot_count = starts_ref.shape
    slot_total = shard_total * slot_count
    heads = query_ref.shape[1] // HS
    factor = 1.0 / math.sqrt(HS)
    used = jnp.sum((starts_ref[...] < byte_count).astype(jnp.int32), axis=1, keepdims=True)
    ids = lax.broadcasted_iota(jnp.int32, (shard_total, slot_total), 1)
    shards = lax.broadcasted_iota(jnp.int32, (shard_total, slot_total), 0)
    inside = ids - shards * slot_count
    usable = jnp.max(
        ((inside >= 0) & (inside < used)).astype(F32), axis=0, keepdims=True
    )
    mine = lax.broadcasted_iota(jnp.int32, (shard_total, 1), 0) == shard
    own_used = jnp.sum(jnp.where(mine, used, 0), axis=0, keepdims=True)
    live = (lax.broadcasted_iota(jnp.int32, (slot_count, 1), 0) < own_used).astype(F32)
    rows = lax.broadcasted_iota(jnp.int32, (slot_count, slot_total), 0) + shard * slot_count
    cols = lax.broadcasted_iota(jnp.int32, (slot_count, slot_total), 1)
    visible = (cols <= rows) & (usable > 0.0)
    keys = both_ref[:, :HS]
    values = both_ref[:, HS:]
    query = stacked(query_ref[...], heads)
    grad = stacked(grad_ref[...], heads)
    live_rows = jnp.concatenate([live] * heads, axis=0)
    seen = jnp.concatenate([visible.astype(F32)] * heads, axis=0) > 0.0
    grad = (grad.astype(F32) * live_rows).astype(BF)
    scores = jnp.where(seen, rows_by_rows(query, keys) * factor, -1e30)
    highest = jnp.max(scores, axis=1, keepdims=True)
    raised = jnp.where(seen, jnp.exp(scores - highest), 0.0)
    total = jnp.maximum(jnp.sum(raised, axis=1, keepdims=True), 1.0)
    attention = raised * (1.0 / total)
    short = attention.astype(BF)
    mixed = rows_by_cols(short, values)
    attended_ref[...] = side_by_side((mixed * live_rows).astype(BF), heads)
    dots = jnp.sum(grad.astype(F32) * mixed, axis=1, keepdims=True)
    prob_grad = rows_by_rows(grad, values)
    score_grad = (attention * ((prob_grad - dots) * factor)).astype(BF)
    query_grad_ref[...] = side_by_side(rows_by_cols(score_grad, keys).astype(BF), heads)
    both_grad_ref[:, :HS] = cols_by_cols(score_grad, query).astype(BF)
    both_grad_ref[:, HS:] = cols_by_cols(short, grad).astype(BF)


def spread_body(parts_ref, pooled_ref, *refs):
    count = len(refs) // 2
    pairs, patch_ref, grad_refs = refs[:count], refs[count], refs[count + 1 :]
    both = gathered_sum(parts_ref).astype(BF)
    xs, _, slots = patch_ref.shape[1:4]
    left = jnp.concatenate([feature_block(pooled_ref, k) for k in range(count)], axis=1)
    weights = jnp.concatenate(
        [jnp.concatenate([pair[0] for pair in pairs], axis=0), jnp.concatenate([pair[1] for pair in pairs], axis=0)],
        axis=1,
    )
    patch = rows_by_rows(both, weights).astype(BF)
    grad = cols_by_cols(left, both).astype(BF)
    for k in range(count):
        y, half = partner(k)
        patch_ref[y, :, half] = patch[:, k * HS : (k + 1) * HS].reshape(xs, slots, HS)
        for which in range(2):
            grad_refs[k][which] = grad[k * HS : (k + 1) * HS, which * HS : (which + 1) * HS]


def total_body(*refs):
    *parts, out_ref = refs
    total = parts[0][...].astype(F32)
    for part in parts[1:]:
        total = total + part[...].astype(F32)
    for copy in range(out_ref.shape[0]):
        out_ref[copy] = total


def add_body(parts_ref, out_ref):
    out_ref[...] = gathered_sum(parts_ref)


def byte_body(starts_ref, parts_ref, out_ref):
    members = members_of(starts_ref, lax.axis_index(BYTE), out_ref.shape[0])
    counts = counts_of(members)
    globs, xs, halves = parts_ref.shape[:3]
    pieces = [None] * (xs * halves)
    for x in range(xs):
        for half in range(halves):
            total = parts_ref[0, x, half].astype(F32)
            for y in range(1, globs):
                total = total + parts_ref[y, x, half].astype(F32)
            pieces[half * xs + x] = (total.astype(BF).astype(F32) / counts).astype(BF)
    out_ref[...] = rows_by_cols(members, jnp.concatenate(pieces, axis=1)).astype(BF)


def on_device(byte_states, patch_start, queries, grad_out, w_kv):
    states = byte_states[0]
    starts = patch_start[0]
    byte_count, width = states.shape
    shard_total, slot_count = starts.shape
    slot_total = shard_total * slot_count
    globs = lax.axis_size("glob")
    depth = lax.axis_size("byte_0")
    across = lax.axis_size("byte_1")
    block = slot_total // depth
    both = 2 * HS
    halves = width // (across * HS)

    pieces = (globs, across, halves, slot_count, HS)

    def around(blocks):
        pairs = [[(z, z ^ k) for z in range(depth)] for k in range(depth)]
        return [blocks[0]] + [lax.ppermute(blocks[k], "byte_0", pairs[k]) for k in range(1, depth)]

    pairs = around([w_kv] * depth)
    send = call(pool_body, shape(pieces), starts, states, name="pool")
    pooled = exchange(send.reshape(-1, *pieces[2:]), CROSS).reshape(pieces)
    send = call(project_body, shape((across, block, both)), pooled, *pairs, name="project")
    parts = exchange(send, "byte_1")
    send = call(share_body, shape((depth, block, both)), parts, name="share")
    key_value = exchange(send, "byte_0").reshape(slot_total, both)
    rows = queries.shape[1:]
    attended, query_grad, send = call(
        functools.partial(attend_body, byte_count=byte_count),
        (shape(rows), shape(rows), shape((slot_total, both))),
        starts, queries[0], grad_out[0], key_value,
        name="attend",
    )
    parts = exchange(send.reshape(depth, block, both), "byte_0")
    send = call(share_body, shape((across, block, both)), parts, name="share_grad")
    parts = exchange(send, "byte_1")
    patch_send, *grads = call(
        spread_body, (shape(pieces), *[shape(w_kv.shape)] * depth), parts, pooled, *pairs, name="spread"
    )
    parts = exchange(patch_send.reshape(-1, *pieces[2:]), CROSS).reshape(pieces)
    byte_grad = call(byte_body, shape((byte_count, width)), starts, parts, name="bytes")
    send = call(total_body, shape((2, *w_kv.shape), F32), *around(grads), name="total")
    pair_grad = call(add_body, shape(w_kv.shape, F32), exchange(send, "dp"), name="sum_dp")
    return (attended[None], query_grad[None], byte_grad[None], pair_grad)


def solution(mesh):
    torus = Mesh(
        mesh.devices.reshape(mesh.shape["dp"], mesh.shape["glob"], 8, 4),
        ("dp", "glob", "byte_0", "byte_1"),
    )
    in_specs = (
        P("dp", BYTE, "glob"),
        P("dp", None, None),
        P("dp", BYTE, "glob"),
        P("dp", BYTE, "glob"),
        P(None, BYTE, "glob"),
    )
    out_specs = (
        P("dp", BYTE, "glob"),
        P("dp", BYTE, "glob"),
        P("dp", BYTE, "glob"),
        P(None, BYTE, "glob"),
    )
    return jax.shard_map(
        on_device, mesh=torus, in_specs=in_specs, out_specs=out_specs, check_vma=False
    )
```
